256 devices in a mesh: replica: 64 (over z, x, core), model: 4 (over y).
Axes of the slice: x: 4, y: 4, z: 8, core: 2. Of those that a mesh axis runs over, the one named last changes fastest.
Arguments:
- partial_query: float32 [64, 1280, 1280], P('replica', None, 'model'), may hold values from -1.75 to 1.75
- partial_key: float32 [64, 1280, 1280], P('replica', None, 'model'), may hold values from -1.75 to 1.75
- partial_value: float32 [64, 1280, 1280], P('replica', None, 'model'), may hold values from -1.75 to 1.75
- partial_mixed: float32 [64, 1280, 1280], P('replica', 'model'), may hold values from -1.75 to 1.75
- partial_norm: float32 [64, 1280], P('replica'), may hold values from -16 to 16
- master_query: float32 [1280, 1280], P('replica', 'model'), may hold values from -0.15625 to 0.15625
- master_key: float32 [1280, 1280], P('replica', 'model'), may hold values from -0.15625 to 0.15625
- master_value: float32 [1280, 1280], P('replica', 'model'), may hold values from -0.15625 to 0.15625
- master_mixed: float32 [1280, 1280], P('model', 'replica'), may hold values from -0.15625 to 0.15625
- master_norm: float32 [1280], P('replica'), may hold values from 0.25 to 1.75
Outputs:
- compute_query: bfloat16 [1280, 1280], P(None, 'model')
- compute_key: bfloat16 [1280, 1280], P(None, 'model')
- compute_value: bfloat16 [1280, 1280], P(None, 'model')
- compute_mixed: bfloat16 [1280, 1280], P('model')
- compute_norm: bfloat16 [1280], replicated
- stepped_query: float32 [1280, 1280], P('replica', 'model')
- stepped_key: float32 [1280, 1280], P('replica', 'model')
- stepped_value: float32 [1280, 1280], P('replica', 'model')
- stepped_mixed: float32 [1280, 1280], P('model', 'replica')
- stepped_norm: float32 [1280], P('replica')
The draws below stay inside these ranges and needn't reach their ends.
All inputs are finite; a program needn't handle non-finite values.
Results may differ from the reference program's by a relative error of at most 0.001.
Values may be sent and summed in bfloat16 or wider, within the bound.
No kernel may reach another device: no remote copies, remote signals or barrier semaphores. Data moves between devices by JAX's collectives and lax.ppermute only.
A program may use at most 128 MiB of HBM per device.

```python
import jax
import jax.numpy as jnp

WIDTH = 1280
ATTN = 1280
REPLICAS = 64


def with_spikes(result, own_key, source, target, parts, factor):
    owner, partner = [(jnp.arange(result.shape[position]) // (result.shape[position] // parts)).reshape([-1 if axis == position else 1 for axis in range(result.ndim)]) for position in (source, target)]
    chosen = jax.random.permutation(own_key, parts)[partner]
    strong = (owner == chosen) | (owner == (partner + parts // 2) % parts)
    return jnp.where(strong, factor * result, result)


def levels(stream_key, shape, cuts, smallest, largest):
    gain = 1.0
    for axis_at, parts in cuts:
        draws = jax.random.uniform(jax.random.fold_in(jax.random.fold_in(stream_key, 6), axis_at), (parts,), jnp.float32, smallest / len(cuts), largest / len(cuts))
        gain = gain * jnp.repeat(jnp.exp(draws), shape[axis_at] // parts).reshape((-1,) + (1,) * (len(shape) - 1 - axis_at))
    return gain


def normal_values(key, extent, spread, most, pieces=(), kind=jnp.bfloat16):
    entries = spread * jax.random.normal(key, extent, jnp.float32)
    if pieces:
        entries = entries * levels(key, extent, pieces, -0.22, 0.18)
    return jnp.clip(entries, -most, most).astype(kind)


def heavy_noise(own_key, dims, spread, most, pieces, heavy, held_as=jnp.bfloat16):
    array = spread * jax.random.normal(own_key, dims, jnp.float32)
    if pieces:
        array = array * levels(own_key, dims, pieces, -0.22, 0.18)
    return jnp.clip(with_spikes(array, jax.random.fold_in(own_key, 3), *heavy), -most, most).astype(held_as)


def setup_inputs(seed: int = 0) -> dict:
    keys = jax.random.split(jax.random.key(seed), 11)
    return {
        "partial_query": heavy_noise(keys[0], (REPLICAS, WIDTH, ATTN), 0.1, 1.75, ((0, 64), (2, 4)), (0, 1, 64, 4.0), jnp.float32),
        "partial_key": heavy_noise(keys[1], (REPLICAS, WIDTH, ATTN), 0.1, 1.75, ((0, 64), (2, 4)), (0, 1, 64, 4.0), jnp.float32),
        "partial_value": heavy_noise(keys[2], (REPLICAS, WIDTH, ATTN), 0.1, 1.75, ((0, 64), (2, 4)), (0, 1, 64, 4.0), jnp.float32),
        "partial_mixed": heavy_noise(keys[3], (REPLICAS, ATTN, WIDTH), 0.1, 1.75, ((0, 64), (1, 4)), (0, 2, 64, 4.0), jnp.float32),
        "partial_norm": heavy_noise(keys[4], (REPLICAS, WIDTH), 1.0, 16.0, ((0, 64),), (0, 1, 64, 4.0), jnp.float32),
        "master_query": normal_values(keys[5], (WIDTH, ATTN), WIDTH ** -0.5, 0.15625, ((0, 64), (1, 4)), jnp.float32),
        "master_key": normal_values(keys[6], (WIDTH, ATTN), WIDTH ** -0.5, 0.15625, ((0, 64), (1, 4)), jnp.float32),
        "master_value": normal_values(keys[7], (WIDTH, ATTN), WIDTH ** -0.5, 0.15625, ((0, 64), (1, 4)), jnp.float32),
        "master_mixed": normal_values(keys[8], (ATTN, WIDTH), ATTN ** -0.5, 0.15625, ((0, 4), (1, 64)), jnp.float32),
        "master_norm": jnp.clip(1.0 + 0.15 * jax.random.normal(keys[9], (WIDTH,), jnp.float32), 0.25, 1.75),
    }


learn_rate = 0.3


def reference(partial_query, partial_key, partial_value, partial_mixed, partial_norm, master_query, master_key, master_value, master_mixed, master_norm):
    mean_query = jnp.sum(partial_query.astype(jnp.float32), axis=0) * REPLICAS ** -0.5
    mean_key = jnp.sum(partial_key.astype(jnp.float32), axis=0) * REPLICAS ** -0.5
    mean_value = jnp.sum(partial_value.astype(jnp.float32), axis=0) * REPLICAS ** -0.5
    mean_mixed = jnp.sum(partial_mixed.astype(jnp.float32), axis=0) * REPLICAS ** -0.5
    mean_norm = jnp.sum(partial_norm.astype(jnp.float32), axis=0) * REPLICAS ** -0.5
    stepped_query = master_query - learn_rate * mean_query
    stepped_key = master_key - learn_rate * mean_key
    stepped_value = master_value - learn_rate * mean_value
    stepped_mixed = master_mixed - learn_rate * mean_mixed
    stepped_norm = master_norm - learn_rate * mean_norm
    compute_query = stepped_query.astype(jnp.bfloat16)
    compute_key = stepped_key.astype(jnp.bfloat16)
    compute_value = stepped_value.astype(jnp.bfloat16)
    compute_mixed = stepped_mixed.astype(jnp.bfloat16)
    compute_norm = stepped_norm.astype(jnp.bfloat16)
    return compute_query, compute_key, compute_value, compute_mixed, compute_norm, stepped_query, stepped_key, stepped_value, stepped_mixed, stepped_norm
```

```python
import jax
import jax.numpy as jnp
from jax import lax
from jax.experimental import pallas as pl
from jax.experimental.pallas import tpu as pltpu
from jax.sharding import Mesh
from jax.sharding import PartitionSpec as P


learn_rate = 0.3
NZ, NX, NC = 8, 4, 2
CHIPS = ("z", "x", "c")
f32, bf16 = jnp.float32, jnp.bfloat16
ROWS, LANES, COLS, COLS_B = 40, 128, 5, 2
A_ROWS = (COLS - COLS_B) * ROWS
B_ROWS = COLS_B * ROWS + 8


def shift(v, dz, dx, dc=0):
    pairs = []
    for z in range(NZ):
        for x in range(NX):
            for c in range(NC):
                there = ((z + dz) % NZ * NX + (x + dx) % NX) * NC + (c ^ dc)
                pairs.append(((z * NX + x) * NC + c, there))
    return lax.ppermute(v, CHIPS, pairs)


def to_core(v, core):
    return lax.ppermute(v, CHIPS, [(i ^ 1, i) for i in range(NZ * NX * NC) if i % 2 == core])


def spread(v):
    return lax.all_to_all(v, "z", 0, 0, tiled=True)


def pair_kernel(who, q, k, v, m, rq, rk, rv, rm, norm, a0, a1, a2, a3, b, own, got, turned, sems):
    core, x = who[0], who[1]

    def copies(first, second, got_first, got_second):
        out = []
        for i in range(2):
            for j, (mine, theirs) in enumerate(((first, got_first), (second, got_second))):
                lanes = pl.ds(640 * i, 640)
                place = pl.ds(320 * j, 320)
                out.append(pltpu.make_async_copy(mine.at[:, lanes], own.at[i, place], sems.at[i, j, 0]))
                out.append(pltpu.make_async_copy(theirs.at[:, lanes], got.at[i, place], sems.at[i, j, 1]))
        return out

    @pl.when(core == 0)
    def _():
        for c in copies(q, k, rq, rk):
            c.start()

    @pl.when(core == 1)
    def _():
        for c in copies(v, m, rv, rm):
            c.start()

    waits = copies(q, k, rq, rk)
    b[:, :, B_ROWS - 8 :, :] = norm[...]
    for i in range(2):
        for c in waits[4 * i : 4 * i + 4]:
            c.wait()
        for t in range(COLS):
            rows = pl.ds(LANES * t, LANES)
            tile = (own[i, rows, :] + got[i, rows, :]).T.reshape(4, NX, ROWS, LANES)
            if t < COLS_B:
                b[4 * i : 4 * i + 4, :, ROWS * t : ROWS * t + ROWS, :] = tile
            else:
                turned[...] = tile
                for j, a in enumerate((a0, a1, a2, a3)):
                    at = ROWS * (t - COLS_B)
                    a[4 * i : 4 * i + 4, at : at + ROWS, :] = turned[:, lax.rem(x + j, NX)]


def vmem(n):
    return [pl.BlockSpec(memory_space=pltpu.VMEM)] * n


def hbm(n):
    return [pl.BlockSpec(memory_space=pl.ANY)] * n


smem = [pl.BlockSpec(memory_space=pltpu.SMEM)]


def first_sum_kernel(who, a0, a1, a2, a3, b, a_out, b0, b1, b2, b3):
    x = who[1]
    a_out[...] = a0[...] + a1[...] + a2[...] + a3[...]
    for j, out in enumerate((b0, b1, b2, b3)):
        at = lax.rem(x + j, NX)
        total = b[0, at]
        for z in range(1, NZ):
            total = total + b[z, at]
        out[...] = total


def step_kernel(a, b0, b1, b2, b3, weight, norm_weight, a_out, b_out, stepped, stepped_norm):
    rate = (NZ * NX * NC) ** (-0.5)
    total_a = a[0]
    for z in range(1, NZ):
        total_a = total_a + a[z]
    total_b = b0[...] + b1[...] + b2[...] + b3[...]
    for t in range(COLS):
        if t < COLS_B:
            total = total_b[ROWS * t : ROWS * t + ROWS]
        else:
            total = total_a[ROWS * (t - COLS_B) : ROWS * (t - COLS_B) + ROWS]
        lanes = slice(LANES * t, LANES * t + LANES)
        new = weight[:, lanes] - learn_rate * (total * rate)
        stepped[:, lanes] = new
        if t < COLS_B:
            b_out[ROWS * t : ROWS * t + ROWS] = new.astype(bf16)
        else:
            for z in range(NZ):
                a_out[z, ROWS * (t - COLS_B) : ROWS * (t - COLS_B) + ROWS] = new.astype(bf16)
    new = norm_weight[...] - learn_rate * (total_b[B_ROWS - 8 :] * rate)
    stepped_norm[...] = new
    b_out[B_ROWS - 8 :] = new.astype(bf16)


def last_kernel(who, a0, a1, a2, a3, b, r0, r1, r2, r3, rb, q, k, v, m, norm, turned):
    core, x = who[0], who[1]
    mine, theirs = ((a0, a1, a2, a3), b), ((r0, r1, r2, r3), rb)
    for j in range(NX):
        for z in range(NZ):
            norm[z, lax.rem(x + NX - j, NX)] = b[z, j, B_ROWS - 8 :, :].astype(f32)
    for flip, (first, second) in enumerate(((q, k), (v, m))):
        for i in range(2):
            for j in range(NX):
                at = lax.rem(x + NX - j, NX) * ROWS
                for z in range(4):
                    rows = pl.ds(pl.multiple_of(at + z * NX * ROWS, 8), ROWS)
                    for t in range(COLS):
                        if t < COLS_B:
                            where = slice(ROWS * t, ROWS * t + ROWS)
                            one, two = b[4 * i + z, j, where, :], rb[4 * i + z, j, where, :]
                        else:
                            where = slice(ROWS * (t - COLS_B), ROWS * (t - COLS_B) + ROWS)
                            one, two = mine[0][j][4 * i + z, where, :], theirs[0][j][4 * i + z, where, :]
                        turned[rows, LANES * t : LANES * t + LANES] = jnp.where(
                            core == flip, one.astype(f32), two.astype(f32)
                        )
            lanes = slice(640 * i, 640 * i + 640)
            for t in range(COLS):
                tile = turned[:, LANES * t : LANES * t + LANES].T.astype(bf16)
                at = LANES * t
                if at + LANES <= 320:
                    first[at : at + LANES, lanes] = tile
                elif at >= 320:
                    second[at - 320 : at - 320 + LANES, lanes] = tile
                else:
                    first[at:320, lanes] = tile[: 320 - at]
                    second[0 : LANES - (320 - at), lanes] = tile[320 - at :]


def on_device(pq, pk, pv, pm, pn, mq, mk, mv, mm, mn):
    core, x = lax.axis_index("c"), lax.axis_index("x")
    who = jnp.stack([core, x]).astype(jnp.int32)
    even = core == 0
    parts = (pq[0].T, pk[0].T, pv[0].T, pm[0])

    got = [to_core(v, 0 if i < 2 else 1) for i, v in enumerate(parts)]
    norm = pn + shift(pn, 0, 0, 1)
    norm = jnp.pad(norm.reshape(NZ, NX, 1, ROWS), ((0, 0), (0, 0), (0, 7), (0, LANES - ROWS)))
    heads, tails = jnp.concatenate([mq, mk], 1), jnp.concatenate([mv, mm.T], 1)
    mine, theirs = jnp.where(even, heads, tails), shift(jnp.where(even, tails, heads), 0, 0, 1)
    weight = jnp.where(even, jnp.concatenate([mine, theirs]), jnp.concatenate([theirs, mine]))
    other = shift(mn, 0, 0, 1)
    norm_weight = jnp.where(even, jnp.concatenate([mn, other]), jnp.concatenate([other, mn]))
    norm_weight = jnp.pad(norm_weight[None], ((0, 7), (0, LANES - ROWS)))

    shape = jax.ShapeDtypeStruct
    a_shape, b_shape = shape((NZ, A_ROWS, LANES), f32), shape((NZ, NX, B_ROWS, LANES), f32)
    *a, b = pl.pallas_call(
        pair_kernel,
        name="pair",
        out_shape=[a_shape] * 4 + [b_shape],
        in_specs=smem + hbm(8) + vmem(1),
        out_specs=vmem(5),
        scratch_shapes=[
            pltpu.VMEM((2, 640, 640), f32),
            pltpu.VMEM((2, 640, 640), f32),
            pltpu.VMEM((4, NX, ROWS, LANES), f32),
            pltpu.SemaphoreType.DMA((2, 2, 2)),
        ],
    )(who, *parts, *got, norm)
    b = spread(b)
    a = [a[0]] + [shift(a[j], 0, j) for j in (1, 2, 3)]
    one = shape((B_ROWS, LANES), f32)
    a, *b = pl.pallas_call(
        first_sum_kernel,
        name="first_sum",
        out_shape=[a_shape] + [one] * 4,
        in_specs=smem + vmem(5),
        out_specs=vmem(5),
    )(who, *a, b)
    a = spread(a)
    b = [b[0]] + [shift(b[j], 0, j) for j in (1, 2, 3)]
    a, b, stepped, stepped_norm = pl.pallas_call(
        step_kernel,
        name="step",
        out_shape=[
            shape((NZ, A_ROWS, LANES), bf16),
            shape((B_ROWS, LANES), bf16),
            shape((ROWS, 640), f32),
            shape((8, LANES), f32),
        ],
        in_specs=vmem(7),
        out_specs=vmem(4),
    )(a, *b, weight, norm_weight)
    stepped_norm = lax.dynamic_slice_in_dim(stepped_norm[0], 20 * core, 20)
    kept = lax.dynamic_slice_in_dim(stepped, 20 * core, 20)
    swapped = shift(lax.dynamic_slice_in_dim(stepped, 20 * (1 - core), 20), 0, 0, 1)
    heads, tails = jnp.where(even, kept, swapped), jnp.where(even, swapped, kept)

    a = spread(a)
    b = jnp.stack([b] + [shift(b, 0, j) for j in (1, 2, 3)])
    b = spread(jnp.broadcast_to(b, (NZ,) + b.shape))
    a = [a] + [shift(a, 0, j) for j in (1, 2, 3)]
    other_a, other_b = [shift(v, 0, 0, 1) for v in a], shift(b, 0, 0, 1)
    wide = shape((320, 1280), bf16)
    q, k, v, m, norm = pl.pallas_call(
        last_kernel,
        name="last",
        out_shape=[wide] * 4 + [shape((NZ, NX, 8, LANES), f32)],
        in_specs=smem + vmem(10),
        out_specs=vmem(5),
        scratch_shapes=[pltpu.VMEM((640, 640), f32)],
    )(who, *a, b, *other_a, other_b)
    return (
        q.T,
        k.T,
        v.T,
        m,
        norm[:, :, 0, :ROWS].reshape(-1).astype(bf16),
        heads[:, :320],
        heads[:, 320:],
        tails[:, :320],
        tails[:, 320:].T,
        stepped_norm,
    )


def solution(mesh):
    split = Mesh(mesh.devices.reshape(NZ, NX, NC, -1), ("z", "x", "c", "model"))
    r = CHIPS
    in_specs = (
        (P(r, None, "model"),) * 3
        + (P(r, "model", None), P(r, None))
        + (P(r, "model"),) * 3
        + (P("model", r), P(r))
    )
    out_specs = (
        (P(None, "model"),) * 3
        + (P("model", None), P())
        + (P(r, "model"),) * 3
        + (P("model", r), P(r))
    )
    return jax.shard_map(
        on_device, mesh=split, in_specs=in_specs, out_specs=out_specs, check_vma=False
    )
```

```python
import jax
import jax.numpy as jnp
from jax import lax
from jax.experimental import pallas as pl
from jax.experimental.pallas import tpu as pltpu
from jax.sharding import Mesh
from jax.sharding import PartitionSpec as P


learn_rate = 0.3
NZ, NX, NC = 8, 4, 2
CHIPS = ("z", "x", "c")
f32, bf16 = jnp.float32, jnp.bfloat16
ROWS, LANES, COLS, COLS_B = 40, 128, 5, 2
A_ROWS = (COLS - COLS_B) * ROWS
B_ROWS = COLS_B * ROWS + 8
SPLIT = COLS_B * LANES


def shift(v, dz, dx, dc=0):
    pairs = []
    for z in range(NZ):
        for x in range(NX):
            for c in range(NC):
                there = ((z + dz) % NZ * NX + (x + dx) % NX) * NC + (c ^ dc)
                pairs.append(((z * NX + x) * NC + c, there))
    return lax.ppermute(v, CHIPS, pairs)


def spread(v):
    return lax.all_to_all(v, "z", 0, 0, tiled=True)


def split_b_kernel(who, q, v, got, norm, b, own, sems):
    def copies(source):
        out = []
        for i in range(2):
            lanes = pl.ds(640 * i, 640)
            place = source.at[pl.ds(0, SPLIT), lanes]
            out.append(pltpu.make_async_copy(place, own.at[:, lanes], sems.at[i]))
        return out

    for core, source in enumerate((q, v)):

        @pl.when(who[0] == core)
        def _(source=source):
            for c in copies(source):
                c.start()

    b[:, :, B_ROWS - 8 :, :] = norm[...]
    for i, c in enumerate(copies(q)):
        c.wait()
        lanes = slice(640 * i, 640 * i + 640)
        for t in range(COLS_B):
            rows = slice(LANES * t, LANES * t + LANES)
            tile = (own[rows, lanes] + got[rows, lanes]).T.reshape(4, NX, ROWS, LANES)
            b[4 * i : 4 * i + 4, :, ROWS * t : ROWS * t + ROWS, :] = tile


def split_a_kernel(who, q, k, v, m, got, a0, a1, a2, a3, own, turned, sems):
    x = who[1]

    def copies(first, second):
        out = []
        for i in range(2):
            lanes = pl.ds(640 * i, 640)
            rest = 320 - SPLIT
            first_rows = first.at[pl.ds(SPLIT, rest), lanes]
            out.append(pltpu.make_async_copy(first_rows, own.at[pl.ds(0, rest), lanes], sems.at[i, 0]))
            out.append(pltpu.make_async_copy(second.at[:, lanes], own.at[pl.ds(rest, 320), lanes], sems.at[i, 1]))
        return out

    for core, pair in enumerate(((q, k), (v, m))):

        @pl.when(who[0] == core)
        def _(pair=pair):
            for c in copies(*pair):
                c.start()

    waits = copies(q, k)
    for i in range(2):
        waits[2 * i].wait()
        waits[2 * i + 1].wait()
        lanes = slice(640 * i, 640 * i + 640)
        for t in range(COLS - COLS_B):
            rows = slice(LANES * t, LANES * t + LANES)
            turned[...] = (own[rows, lanes] + got[rows, lanes]).T.reshape(4, NX, ROWS, LANES)
            for j, a in enumerate((a0, a1, a2, a3)):
                a[4 * i : 4 * i + 4, ROWS * t : ROWS * t + ROWS, :] = turned[:, lax.rem(x + j, NX)]


def vmem(n):
    return [pl.BlockSpec(memory_space=pltpu.VMEM)] * n


def hbm(n):
    return [pl.BlockSpec(memory_space=pl.ANY)] * n


smem = [pl.BlockSpec(memory_space=pltpu.SMEM)]


def near(*arrays):
    return [pltpu.with_memory_space_constraint(v, pltpu.VMEM) for v in arrays]


def first_sum_kernel(who, a0, a1, a2, a3, b, a_out, b0, b1, b2, b3):
    x = who[1]
    a_out[...] = a0[...] + a1[...] + a2[...] + a3[...]
    for j, out in enumerate((b0, b1, b2, b3)):
        at = lax.rem(x + j, NX)
        total = b[0, at]
        for z in range(1, NZ):
            total = total + b[z, at]
        out[...] = total


def step_kernel(a, b0, b1, b2, b3, weight, norm_weight, a_out, b_out, stepped, stepped_norm):
    rate = (NZ * NX * NC) ** (-0.5)
    total_a = a[0]
    for z in range(1, NZ):
        total_a = total_a + a[z]
    total_b = b0[...] + b1[...] + b2[...] + b3[...]
    for t in range(COLS):
        if t < COLS_B:
            total = total_b[ROWS * t : ROWS * t + ROWS]
        else:
            total = total_a[ROWS * (t - COLS_B) : ROWS * (t - COLS_B) + ROWS]
        lanes = slice(LANES * t, LANES * t + LANES)
        new = weight[:, lanes] - learn_rate * (total * rate)
        stepped[:, lanes] = new
        if t < COLS_B:
            b_out[ROWS * t : ROWS * t + ROWS] = new.astype(bf16)
        else:
            for z in range(NZ):
                a_out[z, ROWS * (t - COLS_B) : ROWS * (t - COLS_B) + ROWS] = new.astype(bf16)
    new = norm_weight[...] - learn_rate * (total_b[B_ROWS - 8 :] * rate)
    stepped_norm[...] = new
    b_out[B_ROWS - 8 :] = new.astype(bf16)


def last_kernel(who, a0, a1, a2, a3, b, r0, r1, r2, r3, rb, q, k, v, m, norm, turned):
    core, x = who[0], who[1]
    mine, theirs = ((a0, a1, a2, a3), b), ((r0, r1, r2, r3), rb)
    for j in range(NX):
        for z in range(NZ):
            norm[z, lax.rem(x + NX - j, NX)] = b[z, j, B_ROWS - 8 :, :].astype(f32)
    for flip, (first, second) in enumerate(((q, k), (v, m))):
        for i in range(2):
            for j in range(NX):
                at = lax.rem(x + NX - j, NX) * ROWS
                for z in range(4):
                    rows = pl.ds(pl.multiple_of(at + z * NX * ROWS, 8), ROWS)
                    for t in range(COLS):
                        if t < COLS_B:
                            where = slice(ROWS * t, ROWS * t + ROWS)
                            one, two = b[4 * i + z, j, where, :], rb[4 * i + z, j, where, :]
                        else:
                            where = slice(ROWS * (t - COLS_B), ROWS * (t - COLS_B) + ROWS)
                            one, two = mine[0][j][4 * i + z, where, :], theirs[0][j][4 * i + z, where, :]
                        turned[rows, LANES * t : LANES * t + LANES] = jnp.where(
                            core == flip, one.astype(f32), two.astype(f32)
                        )
            lanes = slice(640 * i, 640 * i + 640)
            for t in range(COLS):
                tile = turned[:, LANES * t : LANES * t + LANES].T.astype(bf16)
                at = LANES * t
                if at + LANES <= 320:
                    first[at : at + LANES, lanes] = tile
                elif at >= 320:
                    second[at - 320 : at - 320 + LANES, lanes] = tile
                else:
                    first[at:320, lanes] = tile[: 320 - at]
                    second[0 : LANES - (320 - at), lanes] = tile[320 - at :]


def on_device(pq, pk, pv, pm, pn, mq, mk, mv, mm, mn):
    core, x = lax.axis_index("c"), lax.axis_index("x")
    who = jnp.stack([core, x]).astype(jnp.int32)
    even = core == 0
    pq, pk, pv, pm = pq[0].T, pk[0].T, pv[0].T, pm[0]
    shape = jax.ShapeDtypeStruct

    norm = pn + shift(pn, 0, 0, 1)
    norm = jnp.pad(norm.reshape(NZ, NX, 1, ROWS), ((0, 0), (0, 0), (0, 7), (0, LANES - ROWS)))
    got_b = shift(jnp.where(even, pv[:SPLIT], pq[:SPLIT]), 0, 0, 1)
    rest = jnp.where(even, jnp.concatenate([pv[SPLIT:], pm]), jnp.concatenate([pq[SPLIT:], pk]))
    got_a = shift(rest, 0, 0, 1)
    heads, tails = jnp.concatenate([mq, mk], 1), jnp.concatenate([mv, mm.T], 1)
    mine, theirs = jnp.where(even, heads, tails), shift(jnp.where(even, tails, heads), 0, 0, 1)
    weight = jnp.where(even, jnp.concatenate([mine, theirs]), jnp.concatenate([theirs, mine]))
    other = shift(mn, 0, 0, 1)
    norm_weight = jnp.where(even, jnp.concatenate([mn, other]), jnp.concatenate([other, mn]))
    norm_weight = jnp.pad(norm_weight[None], ((0, 7), (0, LANES - ROWS)))

    a_shape, b_shape = (NZ, A_ROWS, LANES), (NZ, NX, B_ROWS, LANES)
    b = pl.pallas_call(
        split_b_kernel,
        compiler_params=pltpu.CompilerParams(vmem_limit_bytes=24 << 20),
        name="split_b",
        out_shape=shape(b_shape, f32),
        in_specs=smem + hbm(2) + vmem(2),
        out_specs=vmem(1)[0],
        scratch_shapes=[pltpu.VMEM((SPLIT, 1280), f32), pltpu.SemaphoreType.DMA((2,))],
    )(who, pq, pv, *near(got_b, norm))
    b = spread(b)
    a = pl.pallas_call(
        split_a_kernel,
        compiler_params=pltpu.CompilerParams(vmem_limit_bytes=24 << 20),
        name="split_a",
        out_shape=[pltpu.VMEM(a_shape, f32)] * 4,
        in_specs=smem + hbm(4) + vmem(1),
        out_specs=vmem(4),
        scratch_shapes=[
            pltpu.VMEM((640 - SPLIT, 1280), f32),
            pltpu.VMEM((4, NX, ROWS, LANES), f32),
            pltpu.SemaphoreType.DMA((2, 2)),
        ],
    )(who, pq, pk, pv, pm, *near(got_a))
    a = [a[0]] + [shift(a[j], 0, j) for j in (1, 2, 3)]
    a, b, weight, norm_weight = lax.optimization_barrier((a, b, weight, norm_weight))
    one = pltpu.VMEM((B_ROWS, LANES), f32)
    a, *b = pl.pallas_call(
        first_sum_kernel,
        compiler_params=pltpu.CompilerParams(vmem_limit_bytes=24 << 20),
        name="first_sum",
        out_shape=[pltpu.VMEM(a_shape, f32)] + [one] * 4,
        in_specs=smem + vmem(5),
        out_specs=vmem(5),
    )(who, *near(*a, b))
    a = spread(a)
    b = [b[0]] + [shift(b[j], 0, j) for j in (1, 2, 3)]
    a, b, stepped, stepped_norm = pl.pallas_call(
        step_kernel,
        compiler_params=pltpu.CompilerParams(vmem_limit_bytes=24 << 20),
        name="step",
        out_shape=[
            pltpu.VMEM(a_shape, bf16),
            pltpu.VMEM((B_ROWS, LANES), bf16),
            pltpu.VMEM((ROWS, 640), f32),
            pltpu.VMEM((8, LANES), f32),
        ],
        in_specs=vmem(7),
        out_specs=vmem(4),
    )(*near(a, *b, weight, norm_weight))

    a = spread(a)
    b = jnp.stack([b] + [shift(b, 0, j) for j in (1, 2, 3)])
    a, b = lax.optimization_barrier((a, b))
    stepped_norm = lax.dynamic_slice_in_dim(stepped_norm[0], 20 * core, 20)
    kept = lax.dynamic_slice_in_dim(stepped, 20 * core, 20)
    swapped = shift(lax.dynamic_slice_in_dim(stepped, 20 * (1 - core), 20), 0, 0, 1)
    heads, tails = jnp.where(even, kept, swapped), jnp.where(even, swapped, kept)
    b = spread(jnp.broadcast_to(b, (NZ,) + b.shape))
    a = [a] + [shift(a, 0, j) for j in (1, 2, 3)]
    a, b = lax.optimization_barrier((a, b))
    other_a, other_b = [shift(v, 0, 0, 1) for v in a], shift(b, 0, 0, 1)
    wide = shape((320, 1280), bf16)
    q, k, v, m, norm = pl.pallas_call(
        last_kernel,
        compiler_params=pltpu.CompilerParams(vmem_limit_bytes=24 << 20),
        name="last",
        out_shape=[wide] * 4 + [shape((NZ, NX, 8, LANES), f32)],
        in_specs=smem + vmem(10),
        out_specs=vmem(5),
        scratch_shapes=[pltpu.VMEM((640, 640), f32)],
    )(who, *near(*a, b, *other_a, other_b))
    return (
        q.T,
        k.T,
        v.T,
        m,
        norm[:, :, 0, :ROWS].reshape(-1).astype(bf16),
        heads[:, :320],
        heads[:, 320:],
        tails[:, :320],
        tails[:, 320:].T,
        stepped_norm,
    )


def solution(mesh):
    split = Mesh(mesh.devices.reshape(NZ, NX, NC, -1), ("z", "x", "c", "model"))
    r = CHIPS
    in_specs = (
        (P(r, None, "model"),) * 3
        + (P(r, "model", None), P(r, None))
        + (P(r, "model"),) * 3
        + (P("model", r), P(r))
    )
    out_specs = (
        (P(None, "model"),) * 3
        + (P("model", None), P())
        + (P(r, "model"),) * 3
        + (P("model", r), P(r))
    )
    return jax.shard_map(
        on_device, mesh=split, in_specs=in_specs, out_specs=out_specs, check_vma=False
    )
```

```python
from functools import partial

import jax
import jax.numpy as jnp
from jax import lax
from jax.experimental import pallas as pl
from jax.experimental.pallas import tpu as pltpu
from jax.sharding import Mesh
from jax.sharding import PartitionSpec as P


learn_rate = 0.3
NZ, NX, NC = 8, 4, 2
CHIPS = ("z", "x", "c")
f32, bf16 = jnp.float32, jnp.bfloat16
ROWS, LANES, COLS, EXTRA = 40, 128, 5, 16
B_PIECES = ((0, 0, ROWS, 0), (1, 0, EXTRA, ROWS))
A_PIECES = ((2, 0, ROWS, 0), (3, 0, ROWS, ROWS), (4, 0, ROWS, 2 * ROWS), (1, EXTRA, ROWS, 3 * ROWS))
A_ROWS = 4 * ROWS - EXTRA
B_ROWS = ROWS + EXTRA + 8
G_ROWS = COLS * ROWS + 8
CHUNK = 32
SPLIT = 2 * LANES


def shift(v, dz, dx, dc=0):
    pairs = []
    for z in range(NZ):
        for x in range(NX):
            for c in range(NC):
                there = ((z + dz) % NZ * NX + (x + dx) % NX) * NC + (c ^ dc)
                pairs.append(((z * NX + x) * NC + c, there))
    return lax.ppermute(v, CHIPS, pairs)


def shift_x(v):
    far_one = shift(v[2], 0, 2)
    return [v[0], shift(v[1], 0, 1), far_one, shift(v[3], 0, 3)]


def spread(v):
    return lax.all_to_all(v, "z", 0, 0, tiled=True)


def block_copies(blocks, out, sems, lanes=pl.ds(0, 1280)):
    copies, at = [], 0
    for source, low, count in blocks:
        for r in range(0, count, CHUNK):
            rows, place = pl.ds(low + r, CHUNK), pl.ds(at, CHUNK)
            copies.append(pltpu.make_async_copy(source.at[rows, lanes], out.at[place, lanes], sems.at[at // CHUNK]))
            at += CHUNK
    return copies


def start_for(wanted, pairs, copies_of):
    for core in range(NC):

        @pl.when(lax.axis_index("c") == core)
        def _(core=core):
            for c in copies_of(pairs[wanted(core)]):
                c.start()


def blocks_b(q, v):
    return [[(q, 0, SPLIT)], [(v, 0, SPLIT)]]


def blocks_a(q, k, v, m):
    rest = 320 - SPLIT
    return [[(q, SPLIT, rest), (k, 0, 320)], [(v, SPLIT, rest), (m, 0, 320)]]


def pick_kernel(*refs):
    *sources, send, sems = refs
    pairs = (blocks_b if len(sources) == 2 else blocks_a)(*sources)
    copies_of = lambda blocks: block_copies(blocks, send, sems)
    start_for(lambda core: 1 - core, pairs, copies_of)
    for c in copies_of(pairs[0]):
        c.wait()


HALVES = (pl.ds(0, 640), pl.ds(640, 640))


def split_b_kernel(q, v, got, norm, *refs):
    *outs, extra, own, b, sems, out_sems = refs
    z0 = lax.axis_index("z")
    pairs = blocks_b(q, v)
    halves = lambda blocks: [block_copies(blocks, own, sems.at[i], HALVES[i]) for i in range(2)]
    start_for(lambda core: core, pairs, lambda blocks: sum(halves(blocks), []))
    steps = [lax.rem(z + NZ - z0, NZ) for z in range(NZ)]
    for z, step in enumerate(steps):
        b[step, :, B_ROWS - 8 :, :] = norm[z]
    for i, copies in enumerate(halves(pairs[0])):
        lanes, some = slice(640 * i, 640 * i + 640), slice(4 * i, 4 * i + 4)
        for t in range(2):
            rows = slice(LANES * t, LANES * t + LANES)
            for c in copies[LANES // CHUNK * t : LANES // CHUNK * (t + 1)]:
                c.wait()
            tile = (own[rows, lanes] + got[rows, lanes]).T.reshape(4, NX, ROWS, LANES)
            for z in range(4):
                if t == 0:
                    b[steps[4 * i + z], :, :ROWS, :] = tile[z]
                else:
                    b[steps[4 * i + z], :, ROWS : ROWS + EXTRA, :] = tile[z, :, :EXTRA]
            if t == 1:
                extra[some] = tile[:, :, EXTRA:]
    out_copies = [pltpu.make_async_copy(b.at[r], outs[r], out_sems.at[r]) for r in range(NZ)]
    for c in out_copies:
        c.start()
    for c in out_copies:
        c.wait()


def split_a_kernel(q, k, v, m, got, extra, a0, a1, a2, a3, own, turned, sems):
    x = lax.axis_index("x")
    pairs = blocks_a(q, k, v, m)
    halves = lambda blocks: [block_copies(blocks, own, sems.at[i], HALVES[i]) for i in range(2)]
    start_for(lambda core: core, pairs, lambda blocks: sum(halves(blocks), []))
    for j, a in enumerate((a0, a1, a2, a3)):
        a[:, 3 * ROWS :, :] = extra[:, lax.rem(x + j, NX)]
    for i, copies in enumerate(halves(pairs[0])):
        lanes = slice(640 * i, 640 * i + 640)
        for t in range(3):
            rows = slice(LANES * t, LANES * t + LANES)
            for c in copies[LANES // CHUNK * t : LANES // CHUNK * (t + 1)]:
                c.wait()
            turned[...] = (own[rows, lanes] + got[rows, lanes]).T.reshape(4, NX, ROWS, LANES)
            for j, a in enumerate((a0, a1, a2, a3)):
                a[4 * i : 4 * i + 4, ROWS * t : ROWS * t + ROWS, :] = turned[:, lax.rem(x + j, NX)]


def vmem(n):
    return [pl.BlockSpec(memory_space=pltpu.VMEM)] * n


def hbm(n):
    return [pl.BlockSpec(memory_space=pltpu.HBM)] * n


FAR = pltpu.HBM


def near(*arrays):
    return [pltpu.with_memory_space_constraint(v, pltpu.VMEM) for v in arrays]


def far(*arrays):
    return [pltpu.with_memory_space_constraint(v, pltpu.HBM) for v in arrays]


def sum_a_kernel(a0, a1, a2, a3, out, own, sem):
    copy = pltpu.make_async_copy(a0, own, sem)
    copy.start()
    copy.wait()
    out[...] = own[...] + a1[...] + a2[...] + a3[...]


def sum_b_kernel(*refs):
    first, rest, outs, own, sem = refs[0], refs[1:NZ], refs[NZ:-2], refs[-2], refs[-1]
    x = lax.axis_index("x")
    copy = pltpu.make_async_copy(first, own, sem)
    copy.start()
    copy.wait()
    for j, out in enumerate(outs):
        at = lax.rem(x + j, NX)
        total = own[at]
        for b in rest:
            total = total + b[at]
        out[...] = total


def step_kernel(a, b0, b1, b2, b3, weight, norm_weight, out, stepped, stepped_norm):
    rate = (NZ * NX * NC) ** (-0.5)
    total_a = a[0]
    for z in range(1, NZ):
        total_a = total_a + a[z]
    total_b = b0[...] + b1[...] + b2[...] + b3[...]
    for pieces, total in ((B_PIECES, total_b), (A_PIECES, total_a)):
        for t, low, high, at in pieces:
            lanes, place = slice(LANES * t, LANES * t + LANES), slice(at, at + high - low)
            stepped[low:high, lanes] = weight[low:high, lanes] - learn_rate * (total[place] * rate)
    stepped_norm[...] = norm_weight[...] - learn_rate * (total_b[B_ROWS - 8 :] * rate)
    for t in range(COLS):
        new = stepped[:, LANES * t : LANES * t + LANES].astype(bf16)
        for z in range(NZ):
            out[z, ROWS * t : ROWS * t + ROWS] = new
    new = stepped_norm[...].astype(bf16)
    for z in range(NZ):
        out[z, G_ROWS - 8 :] = new


def turn_kernel(own, a0, a1, a2, a3, *refs):
    q, k, v, m, turned, pair, sems = refs[-7:]
    core, x = lax.axis_index("c"), lax.axis_index("x")
    pairs = ((q, k), (v, m))

    def copies(i, pair_out):
        lanes = HALVES[i]
        return [
            pltpu.make_async_copy(pair.at[pl.ds(320 * j, 320), lanes], out.at[:, lanes], sems.at[i, j])
            for j, out in enumerate(pair_out)
        ]

    for i in range(2):
        for j, a in enumerate((a0, a1, a2, a3)):
            place = lax.rem(x + NX - j, NX) * ROWS
            for z in range(4):
                rows = pl.ds(pl.multiple_of(place + z * NX * ROWS, 8), ROWS)
                for t in range(COLS):
                    tile = a[4 * i + z, ROWS * t : ROWS * t + ROWS, :]
                    turned[rows, LANES * t : LANES * t + LANES] = tile.astype(f32)
        for t in range(COLS):
            lanes = slice(LANES * t, LANES * t + LANES)
            pair[lanes, 640 * i : 640 * i + 640] = turned[:, lanes].T.astype(bf16)
        for flip in range(2):

            @pl.when(core == (flip if own else 1 - flip))
            def _(flip=flip):
                for c in copies(i, pairs[flip]):
                    c.start()

    for i in range(2):
        for c in copies(i, pairs[0]):
            c.wait()


def call(kernel, out_shape, in_specs, scratch=(), out_specs=None, aliases={}):
    return pl.pallas_call(
        kernel,
        compiler_params=pltpu.CompilerParams(vmem_limit_bytes=24 << 20),
        out_shape=out_shape,
        in_specs=in_specs,
        out_specs=out_specs or jax.tree.map(lambda _: vmem(1)[0], out_shape),
        input_output_aliases=aliases,
        scratch_shapes=scratch,
    )


def on_device(pq, pk, pv, pm, pn, mq, mk, mv, mm, mn):
    core, x = lax.axis_index("c"), lax.axis_index("x")
    even = core == 0
    pq, pk, pv, pm = pq[0].T, pk[0].T, pv[0].T, pm[0]
    dma = pltpu.SemaphoreType.DMA

    norm = shift(pn, 0, 0, 1)
    norm = pn + norm
    norm = jnp.pad(norm.reshape(NZ, NX, 1, ROWS), ((0, 0), (0, 0), (0, 7), (0, LANES - ROWS)))
    chunks_b, chunks_a = SPLIT // CHUNK, (640 - SPLIT) // CHUNK
    send_b = call(
        pick_kernel, pltpu.VMEM((SPLIT, 1280), f32), hbm(2), [dma((chunks_b,))]
    )(*far(pq, pv))
    got_b = shift(send_b, 0, 0, 1)
    send_a = call(
        pick_kernel, pltpu.VMEM((640 - SPLIT, 1280), f32), hbm(4), [dma((chunks_a,))]
    )(*far(pq, pk, pv, pm))
    got_a = shift(send_a, 0, 0, 1)
    heads, tails = jnp.concatenate([mq, mk], 1), jnp.concatenate([mv, mm.T], 1)
    mine, theirs = jnp.where(even, heads, tails), shift(jnp.where(even, tails, heads), 0, 0, 1)
    weight = jnp.where(even, jnp.concatenate([mine, theirs]), jnp.concatenate([theirs, mine]))
    other = shift(mn, 0, 0, 1)
    norm_weight = jnp.where(even, jnp.concatenate([mn, other]), jnp.concatenate([other, mn]))
    norm_weight = jnp.pad(norm_weight[None], ((0, 7), (0, LANES - ROWS)))

    a_shape, b_shape = (NZ, A_ROWS, LANES), (NX, B_ROWS, LANES)
    *b, extra = call(
        split_b_kernel,
        [FAR(b_shape, f32)] * NZ + [pltpu.VMEM((NZ, NX, ROWS - EXTRA, LANES), f32)],
        hbm(2) + vmem(2),
        [pltpu.VMEM((SPLIT, 1280), f32), pltpu.VMEM((NZ, *b_shape), f32), dma((2, chunks_b)), dma((NZ,))],
        hbm(NZ) + vmem(1),
    )(*far(pq, pv), *near(got_b, norm))
    got = [b[0]]
    for steps in ((3, 5), (2, 6, 4, 1, 7)):
        got += [shift(b[r], r, 0) for r in steps]
    b = got
    a = call(
        split_a_kernel,
        [FAR(a_shape, f32)] + [pltpu.VMEM(a_shape, f32)] * 3,
        hbm(4) + vmem(2),
        [
            pltpu.VMEM((640 - SPLIT, 1280), f32),
            pltpu.VMEM((4, NX, ROWS, LANES), f32),
            dma((2, chunks_a)),
        ],
    )(*far(pq, pk, pv, pm), *near(got_a, extra))
    a = shift_x(a)
    a, b, weight, norm_weight = lax.optimization_barrier((a, b, weight, norm_weight))
    a = call(
        sum_a_kernel, pltpu.VMEM(a_shape, f32), hbm(1) + vmem(3), [pltpu.VMEM(a_shape, f32), dma]
    )(*far(a[0]), *near(*a[1:]))
    a = spread(a)
    b = call(
        sum_b_kernel,
        [pltpu.VMEM((B_ROWS, LANES), f32)] * NX,
        hbm(1) + vmem(NZ - 1),
        [pltpu.VMEM(b_shape, f32), dma],
    )(*far(b[0]), *near(*b[1:]))
    b = [b[0]] + [shift(b[j], 0, j) for j in (1, 2, 3)]
    a, stepped, stepped_norm = call(
        step_kernel,
        [
            pltpu.VMEM((NZ, G_ROWS, LANES), bf16),
            pltpu.VMEM((ROWS, 640), f32),
            pltpu.VMEM((8, LANES), f32),
        ],
        vmem(7),
    )(*near(a, *b, weight, norm_weight))

    a = spread(a)
    a = shift_x([a] * NX)
    stepped_norm = lax.dynamic_slice_in_dim(stepped_norm[0], 20 * core, 20)
    kept = lax.dynamic_slice_in_dim(stepped, 20 * core, 20)
    swapped = shift(lax.dynamic_slice_in_dim(stepped, 20 * (1 - core), 20), 0, 0, 1)
    heads, tails = jnp.where(even, kept, swapped), jnp.where(even, swapped, kept)
    outs = (heads[:, :320], heads[:, 320:], tails[:, :320], tails[:, 320:].T, stepped_norm)
    a[3], outs = lax.optimization_barrier((a[3], outs))
    other_a = [shift(v, 0, 0, 1) for v in a]
    own_x = jnp.arange(NX)[:, None]
    norm = sum(
        jnp.where(own_x == lax.rem(x + NX - j, NX), v[:, None, G_ROWS - 8, :ROWS], 0) for j, v in enumerate(a)
    )
    scratch = [pltpu.VMEM((640, 640), f32), pltpu.VMEM((640, 1280), bf16), dma((2, 2))]
    outs_shape = [FAR((320, 1280), bf16)] * 4
    half = call(partial(turn_kernel, True), outs_shape, vmem(4), scratch, hbm(4))(*near(*a))
    aliases = {4 + i: i for i in range(4)}
    q, k, v, m = call(
        partial(turn_kernel, False), outs_shape, vmem(4) + hbm(4), scratch, hbm(4), aliases
    )(*near(*other_a), *half)
    return (q.T, k.T, v.T, m, norm.reshape(-1).astype(bf16), *outs)


def solution(mesh):
    split = Mesh(mesh.devices.reshape(NZ, NX, NC, -1), ("z", "x", "c", "model"))
    r = CHIPS
    in_specs = (
        (P(r, None, "model"),) * 3
        + (P(r, "model", None), P(r, None))
        + (P(r, "model"),) * 3
        + (P("model", r), P(r))
    )
    out_specs = (
        (P(None, "model"),) * 3
        + (P("model", None), P())
        + (P(r, "model"),) * 3
        + (P("model", r), P(r))
    )
    return jax.shard_map(
        on_device, mesh=split, in_specs=in_specs, out_specs=out_specs, check_vma=False
    )
```

```python
from functools import partial

import jax
import jax.numpy as jnp
from jax import lax
from jax.experimental import pallas as pl
from jax.experimental.pallas import tpu as pltpu
from jax.sharding import Mesh
from jax.sharding import PartitionSpec as P


learn_rate = 0.3
NZ, NX, NC = 8, 4, 2
CHIPS = ("z", "x", "c")
f32, bf16 = jnp.float32, jnp.bfloat16
ROWS, LANES, COLS = 40, 128, 5
A_ROWS, B_ROWS, SPLIT = 4 * ROWS, ROWS + 8, LANES
G_ROWS = COLS * ROWS + 8
CHUNK = 32


def shift(v, dz, dx, dc=0):
    pairs = []
    for z in range(NZ):
        for x in range(NX):
            for c in range(NC):
                there = ((z + dz) % NZ * NX + (x + dx) % NX) * NC + (c ^ dc)
                pairs.append(((z * NX + x) * NC + c, there))
    return lax.ppermute(v, CHIPS, pairs)


def shift_x(v):
    far_one = shift(v[2], 0, 2)
    return [v[0], shift(v[1], 0, 1), far_one, shift(v[3], 0, 3)]


def spread(v):
    return lax.all_to_all(v, "z", 0, 0, tiled=True)


def block_copies(blocks, out, sems, lanes=pl.ds(0, 1280)):
    copies, at = [], 0
    for source, low, count in blocks:
        for r in range(0, count, CHUNK):
            rows, place = pl.ds(low + r, CHUNK), pl.ds(at, CHUNK)
            copies.append(pltpu.make_async_copy(source.at[rows, lanes], out.at[place, lanes], sems.at[at // CHUNK]))
            at += CHUNK
    return copies


def start_for(wanted, pairs, copies_of):
    for core in range(NC):

        @pl.when(lax.axis_index("c") == core)
        def _(core=core):
            for c in copies_of(pairs[wanted(core)]):
                c.start()


def blocks_b(q, v):
    return [[(q, 0, SPLIT)], [(v, 0, SPLIT)]]


def blocks_a(q, k, v, m):
    rest = 320 - SPLIT
    return [[(q, SPLIT, rest), (k, 0, 320)], [(v, SPLIT, rest), (m, 0, 320)]]


def pick_kernel(*refs):
    *sources, send, sems = refs
    pairs = (blocks_b if len(sources) == 2 else blocks_a)(*sources)
    copies_of = lambda blocks: block_copies(blocks, send, sems)
    start_for(lambda core: 1 - core, pairs, copies_of)
    for c in copies_of(pairs[0]):
        c.wait()


HALVES = (pl.ds(0, 640), pl.ds(640, 640))


def split_b_kernel(q, v, got, norm, *refs):
    *outs, own, b, sems, out_sems = refs
    z0 = lax.axis_index("z")
    pairs = blocks_b(q, v)
    halves = lambda blocks: [block_copies(blocks, own, sems.at[i], HALVES[i]) for i in range(2)]
    start_for(lambda core: core, pairs, lambda blocks: sum(halves(blocks), []))
    steps = [lax.rem(z + NZ - z0, NZ) for z in range(NZ)]
    for z, step in enumerate(steps):
        b[step, :, B_ROWS - 8 :, :] = norm[z]
    for i, copies in enumerate(halves(pairs[0])):
        for c in copies:
            c.wait()
        lanes = slice(640 * i, 640 * i + 640)
        tile = (own[:, lanes] + got[:, lanes]).T.reshape(4, NX, ROWS, LANES)
        for z in range(4):
            b[steps[4 * i + z], :, :ROWS, :] = tile[z]
    out_copies = [pltpu.make_async_copy(b.at[r], outs[r], out_sems.at[r]) for r in range(NZ)]
    for c in out_copies:
        c.start()
    for c in out_copies:
        c.wait()


def split_a_kernel(q, k, v, m, got, a0, a1, a2, a3, own, turned, sems):
    x = lax.axis_index("x")
    pairs = blocks_a(q, k, v, m)
    halves = lambda blocks: [block_copies(blocks, own, sems.at[i], HALVES[i]) for i in range(2)]
    start_for(lambda core: core, pairs, lambda blocks: sum(halves(blocks), []))
    for i, copies in enumerate(halves(pairs[0])):
        lanes = slice(640 * i, 640 * i + 640)
        for t in range(COLS - 1):
            rows = slice(LANES * t, LANES * t + LANES)
            for c in copies[LANES // CHUNK * t : LANES // CHUNK * (t + 1)]:
                c.wait()
            turned[...] = (own[rows, lanes] + got[rows, lanes]).T.reshape(4, NX, ROWS, LANES)
            for j, a in enumerate((a0, a1, a2, a3)):
                a[4 * i : 4 * i + 4, ROWS * t : ROWS * t + ROWS, :] = turned[:, lax.rem(x + j, NX)]


def vmem(n):
    return [pl.BlockSpec(memory_space=pltpu.VMEM)] * n


def hbm(n):
    return [pl.BlockSpec(memory_space=pltpu.HBM)] * n


FAR = pltpu.HBM


def near(*arrays):
    return [pltpu.with_memory_space_constraint(v, pltpu.VMEM) for v in arrays]


def far(*arrays):
    return [pltpu.with_memory_space_constraint(v, pltpu.HBM) for v in arrays]


def sum_a_kernel(a0, a1, a2, a3, out, own, sem):
    copy = pltpu.make_async_copy(a0, own, sem)
    copy.start()
    copy.wait()
    out[...] = own[...] + a1[...] + a2[...] + a3[...]


def sum_b_kernel(*refs):
    first, rest, outs, own, sem = refs[0], refs[1:NZ], refs[NZ:-2], refs[-2], refs[-1]
    x = lax.axis_index("x")
    copy = pltpu.make_async_copy(first, own, sem)
    copy.start()
    copy.wait()
    for j, out in enumerate(outs):
        at = lax.rem(x + j, NX)
        total = own[at]
        for b in rest:
            total = total + b[at]
        out[...] = total


def step_kernel(a, b0, b1, b2, b3, weight, norm_weight, out, stepped, stepped_norm):
    rate = (NZ * NX * NC) ** (-0.5)
    total_a = a[0]
    for z in range(1, NZ):
        total_a = total_a + a[z]
    total_b = b0[...] + b1[...] + b2[...] + b3[...]
    for t in range(COLS):
        lanes = slice(LANES * t, LANES * t + LANES)
        total = total_b[:ROWS] if t == 0 else total_a[ROWS * (t - 1) : ROWS * t]
        stepped[:, lanes] = weight[:, lanes] - learn_rate * (total * rate)
    stepped_norm[...] = norm_weight[...] - learn_rate * (total_b[B_ROWS - 8 :] * rate)
    for t in range(COLS):
        new = stepped[:, LANES * t : LANES * t + LANES].astype(bf16)
        for z in range(NZ):
            out[z, ROWS * t : ROWS * t + ROWS] = new
    new = stepped_norm[...].astype(bf16)
    for z in range(NZ):
        out[z, G_ROWS - 8 :] = new


def turn_kernel(own, a0, a1, a2, a3, *refs):
    q, k, v, m, turned, pair, sems = refs[-7:]
    core, x = lax.axis_index("c"), lax.axis_index("x")
    pairs = ((q, k), (v, m))

    def copies(i, pair_out):
        lanes = HALVES[i]
        return [
            pltpu.make_async_copy(pair.at[pl.ds(320 * j, 320), lanes], out.at[:, lanes], sems.at[i, j])
            for j, out in enumerate(pair_out)
        ]

    for i in range(2):
        for j, a in enumerate((a0, a1, a2, a3)):
            place = lax.rem(x + NX - j, NX) * ROWS
            for z in range(4):
                rows = pl.ds(pl.multiple_of(place + z * NX * ROWS, 8), ROWS)
                for t in range(COLS):
                    tile = a[4 * i + z, ROWS * t : ROWS * t + ROWS, :]
                    turned[rows, LANES * t : LANES * t + LANES] = tile.astype(f32)
        for t in range(COLS):
            lanes = slice(LANES * t, LANES * t + LANES)
            pair[lanes, 640 * i : 640 * i + 640] = turned[:, lanes].T.astype(bf16)
        for flip in range(2):

            @pl.when(core == (flip if own else 1 - flip))
            def _(flip=flip):
                for c in copies(i, pairs[flip]):
                    c.start()

    for i in range(2):
        for c in copies(i, pairs[0]):
            c.wait()


def call(kernel, out_shape, in_specs, scratch=(), out_specs=None, aliases={}):
    return pl.pallas_call(
        kernel,
        compiler_params=pltpu.CompilerParams(vmem_limit_bytes=24 << 20),
        out_shape=out_shape,
        in_specs=in_specs,
        out_specs=out_specs or jax.tree.map(lambda _: vmem(1)[0], out_shape),
        input_output_aliases=aliases,
        scratch_shapes=scratch,
    )


def on_device(pq, pk, pv, pm, pn, mq, mk, mv, mm, mn):
    core, x = lax.axis_index("c"), lax.axis_index("x")
    even = core == 0
    pq, pk, pv, pm = pq[0].T, pk[0].T, pv[0].T, pm[0]
    dma = pltpu.SemaphoreType.DMA

    norm = shift(pn, 0, 0, 1)
    norm = pn + norm
    norm = jnp.pad(norm.reshape(NZ, NX, 1, ROWS), ((0, 0), (0, 0), (0, 7), (0, LANES - ROWS)))
    chunks_b, chunks_a = SPLIT // CHUNK, (640 - SPLIT) // CHUNK
    send_b = call(
        pick_kernel, pltpu.VMEM((SPLIT, 1280), f32), hbm(2), [dma((chunks_b,))]
    )(*far(pq, pv))
    got_b = shift(send_b, 0, 0, 1)
    send_a = call(
        pick_kernel, pltpu.VMEM((640 - SPLIT, 1280), f32), hbm(4), [dma((chunks_a,))]
    )(*far(pq, pk, pv, pm))
    got_a = shift(send_a, 0, 0, 1)
    heads, tails = jnp.concatenate([mq, mk], 1), jnp.concatenate([mv, mm.T], 1)
    mine, theirs = jnp.where(even, heads, tails), jnp.where(even, tails, heads)
    theirs, other = shift(theirs, 0, 0, 1), shift(mn, 0, 0, 1)
    weight = jnp.where(even, jnp.concatenate([mine, theirs]), jnp.concatenate([theirs, mine]))
    norm_weight = jnp.where(even, jnp.concatenate([mn, other]), jnp.concatenate([other, mn]))
    norm_weight = jnp.pad(norm_weight[None], ((0, 7), (0, LANES - ROWS)))

    a_shape, b_shape = (NZ, A_ROWS, LANES), (NX, B_ROWS, LANES)
    b = call(
        split_b_kernel,
        [FAR(b_shape, f32)] * NZ,
        hbm(2) + vmem(2),
        [pltpu.VMEM((SPLIT, 1280), f32), pltpu.VMEM((NZ, *b_shape), f32), dma((2, chunks_b)), dma((NZ,))],
        hbm(NZ),
    )(*far(pq, pv), *near(got_b, norm))
    got = [b[0]]
    for steps in ((2, 6), (3, 5, 4, 1, 7)):
        got += [shift(b[r], r, 0) for r in steps]
    b = got
    a = call(
        split_a_kernel,
        [FAR(a_shape, f32)] + [pltpu.VMEM(a_shape, f32)] * 3,
        hbm(4) + vmem(1),
        [
            pltpu.VMEM((640 - SPLIT, 1280), f32),
            pltpu.VMEM((4, NX, ROWS, LANES), f32),
            dma((2, chunks_a)),
        ],
    )(*far(pq, pk, pv, pm), *near(got_a))
    a = shift_x(a)
    a, b, weight, norm_weight = lax.optimization_barrier((a, b, weight, norm_weight))
    a = call(
        sum_a_kernel, pltpu.VMEM(a_shape, f32), hbm(1) + vmem(3), [pltpu.VMEM(a_shape, f32), dma]
    )(*far(a[0]), *near(*a[1:]))
    a = spread(a)
    b = call(
        sum_b_kernel,
        [pltpu.VMEM((B_ROWS, LANES), f32)] * NX,
        hbm(1) + vmem(NZ - 1),
        [pltpu.VMEM(b_shape, f32), dma],
    )(*far(b[0]), *near(*b[1:]))
    b = [b[0]] + [shift(b[j], 0, j) for j in (1, 2, 3)]
    a, stepped, stepped_norm = call(
        step_kernel,
        [
            pltpu.VMEM((NZ, G_ROWS, LANES), bf16),
            pltpu.VMEM((ROWS, 640), f32),
            pltpu.VMEM((8, LANES), f32),
        ],
        vmem(7),
    )(*near(a, *b, weight, norm_weight))

    a = spread(a)
    a = shift_x([a] * NX)
    stepped_norm = lax.dynamic_slice_in_dim(stepped_norm[0], 20 * core, 20)
    kept = lax.dynamic_slice_in_dim(stepped, 20 * core, 20)
    swapped = shift(lax.dynamic_slice_in_dim(stepped, 20 * (1 - core), 20), 0, 0, 1)
    heads, tails = jnp.where(even, kept, swapped), jnp.where(even, swapped, kept)
    outs = (heads[:, :320], heads[:, 320:], tails[:, :320], tails[:, 320:].T, stepped_norm)
    a[3], outs = lax.optimization_barrier((a[3], outs))
    other_a = [shift(v, 0, 0, 1) for v in a]
    own_x = jnp.arange(NX)[:, None]
    norm = sum(
        jnp.where(own_x == lax.rem(x + NX - j, NX), v[:, None, G_ROWS - 8, :ROWS], 0) for j, v in enumerate(a)
    )
    scratch = [pltpu.VMEM((640, 640), f32), pltpu.VMEM((640, 1280), bf16), dma((2, 2))]
    outs_shape = [FAR((320, 1280), bf16)] * 4
    half = call(partial(turn_kernel, True), outs_shape, vmem(4), scratch, hbm(4))(*near(*a))
    aliases = {4 + i: i for i in range(4)}
    q, k, v, m = call(
        partial(turn_kernel, False), outs_shape, vmem(4) + hbm(4), scratch, hbm(4), aliases
    )(*near(*other_a), *half)
    return (q.T, k.T, v.T, m, norm.reshape(-1).astype(bf16), *outs)


def solution(mesh):
    split = Mesh(mesh.devices.reshape(NZ, NX, NC, -1), ("z", "x", "c", "model"))
    r = CHIPS
    in_specs = (
        (P(r, None, "model"),) * 3
        + (P(r, "model", None), P(r, None))
        + (P(r, "model"),) * 3
        + (P("model", r), P(r))
    )
    out_specs = (
        (P(None, "model"),) * 3
        + (P("model", None), P())
        + (P(r, "model"),) * 3
        + (P("model", r), P(r))
    )
    return jax.shard_map(
        on_device, mesh=split, in_specs=in_specs, out_specs=out_specs, check_vma=False
    )
```

```python
from functools import partial

import jax
import jax.numpy as jnp
from jax import lax
from jax.experimental import pallas as pl
from jax.experimental.pallas import tpu as pltpu
from jax.sharding import Mesh
from jax.sharding import PartitionSpec as P


learn_rate = 0.3
NZ, NX, NC = 8, 4, 2
CHIPS = ("z", "x", "c")
f32, bf16 = jnp.float32, jnp.bfloat16
ROWS, LANES, COLS = 40, 128, 5
A_ROWS, B_ROWS, SPLIT = 4 * ROWS, ROWS + 8, LANES
G_ROWS = COLS * ROWS + 8
CHUNK = 32


def shift(v, dz, dx, dc=0):
    pairs = []
    for z in range(NZ):
        for x in range(NX):
            for c in range(NC):
                there = ((z + dz) % NZ * NX + (x + dx) % NX) * NC + (c ^ dc)
                pairs.append(((z * NX + x) * NC + c, there))
    return lax.ppermute(v, CHIPS, pairs)


def shift_x(v):
    near_ones = shift(v[1], 0, 1), shift(v[3], 0, 3)
    return [v[0], near_ones[0], shift(v[2], 0, 2), near_ones[1]]


def spread(v):
    return lax.all_to_all(v, "z", 0, 0, tiled=True)


def block_copies(blocks, out, sems, lanes=pl.ds(0, 1280)):
    copies, at = [], 0
    for source, low, count in blocks:
        for r in range(0, count, CHUNK):
            rows, place = pl.ds(low + r, CHUNK), pl.ds(at, CHUNK)
            copies.append(pltpu.make_async_copy(source.at[rows, lanes], out.at[place, lanes], sems.at[at // CHUNK]))
            at += CHUNK
    return copies


def start_for(wanted, pairs, copies_of):
    for core in range(NC):

        @pl.when(lax.axis_index("c") == core)
        def _(core=core):
            for c in copies_of(pairs[wanted(core)]):
                c.start()


def blocks_b(q, v):
    return [[(q, 0, SPLIT)], [(v, 0, SPLIT)]]


def blocks_a(q, k, v, m):
    rest = 320 - SPLIT
    return [[(q, SPLIT, rest), (k, 0, 320)], [(v, SPLIT, rest), (m, 0, 320)]]


def pick_kernel(*refs):
    *sources, send, sems = refs
    pairs = (blocks_b if len(sources) == 2 else blocks_a)(*sources)
    copies_of = lambda blocks: block_copies(blocks, send, sems)
    start_for(lambda core: 1 - core, pairs, copies_of)
    for c in copies_of(pairs[0]):
        c.wait()


HALVES = (pl.ds(0, 640), pl.ds(640, 640))


def split_b_kernel(q, v, got, norm, *refs):
    *outs, own, b, sems, out_sems = refs
    z0 = lax.axis_index("z")
    pairs = blocks_b(q, v)
    halves = lambda blocks: [block_copies(blocks, own, sems.at[i], HALVES[i]) for i in range(2)]
    start_for(lambda core: core, pairs, lambda blocks: sum(halves(blocks), []))
    steps = [lax.rem(z + NZ - z0, NZ) for z in range(NZ)]
    for z, step in enumerate(steps):
        b[step, :, B_ROWS - 8 :, :] = norm[z]
    for i, copies in enumerate(halves(pairs[0])):
        for c in copies:
            c.wait()
        lanes = slice(640 * i, 640 * i + 640)
        tile = (own[:, lanes] + got[:, lanes]).T.reshape(4, NX, ROWS, LANES)
        for z in range(4):
            b[steps[4 * i + z], :, :ROWS, :] = tile[z]
    out_copies = [pltpu.make_async_copy(b.at[r], outs[r], out_sems.at[r]) for r in range(NZ)]
    for c in out_copies:
        c.start()
    for c in out_copies:
        c.wait()


def split_a_kernel(q, k, v, m, got, a0, a1, a2, a3, own, turned, sems):
    x = lax.axis_index("x")
    pairs = blocks_a(q, k, v, m)
    halves = lambda blocks: [block_copies(blocks, own, sems.at[i], HALVES[i]) for i in range(2)]
    start_for(lambda core: core, pairs, lambda blocks: sum(halves(blocks), []))
    for i, copies in enumerate(halves(pairs[0])):
        lanes = slice(640 * i, 640 * i + 640)
        for t in range(COLS - 1):
            rows = slice(LANES * t, LANES * t + LANES)
            for c in copies[LANES // CHUNK * t : LANES // CHUNK * (t + 1)]:
                c.wait()
            turned[...] = (own[rows, lanes] + got[rows, lanes]).T.reshape(4, NX, ROWS, LANES)
            for j, a in enumerate((a0, a1, a2, a3)):
                a[4 * i : 4 * i + 4, ROWS * t : ROWS * t + ROWS, :] = turned[:, lax.rem(x + j, NX)]


def vmem(n):
    return [pl.BlockSpec(memory_space=pltpu.VMEM)] * n


def hbm(n):
    return [pl.BlockSpec(memory_space=pltpu.HBM)] * n


FAR = pltpu.HBM


def near(*arrays):
    return [pltpu.with_memory_space_constraint(v, pltpu.VMEM) for v in arrays]


def far(*arrays):
    return [pltpu.with_memory_space_constraint(v, pltpu.HBM) for v in arrays]


def sum_a_kernel(a0, a1, a2, a3, out, own, sems):
    copies = [pltpu.make_async_copy(a0.at[z], own.at[z], sems.at[z]) for z in range(NZ)]
    for c in copies:
        c.start()
    for z, c in enumerate(copies):
        c.wait()
        out[z] = own[z] + a1[z] + a2[z] + a3[z]


def sum_b_kernel(*refs):
    first, rest, outs, own, sem = refs[0], refs[1:NZ], refs[NZ:-2], refs[-2], refs[-1]
    x = lax.axis_index("x")
    copy = pltpu.make_async_copy(first, own, sem)
    copy.start()
    copy.wait()
    for j, out in enumerate(outs):
        at = lax.rem(x + j, NX)
        total = own[at]
        for b in rest:
            total = total + b[at]
        out[...] = total


def step_kernel(a, b0, b1, b2, b3, weight, norm_weight, out, stepped, stepped_norm):
    rate = (NZ * NX * NC) ** (-0.5)
    total_a = a[0]
    for z in range(1, NZ):
        total_a = total_a + a[z]
    total_b = b0[...] + b1[...] + b2[...] + b3[...]
    for t in range(COLS):
        lanes = slice(LANES * t, LANES * t + LANES)
        total = total_b[:ROWS] if t == 0 else total_a[ROWS * (t - 1) : ROWS * t]
        stepped[:, lanes] = weight[:, lanes] - learn_rate * (total * rate)
    stepped_norm[...] = norm_weight[...] - learn_rate * (total_b[B_ROWS - 8 :] * rate)
    for t in range(COLS):
        out[ROWS * t : ROWS * t + ROWS] = stepped[:, LANES * t : LANES * t + LANES].astype(bf16)
    out[G_ROWS - 8 :] = stepped_norm[...].astype(bf16)


def turn_kernel(own, a0, a1, a2, a3, *refs):
    q, k, v, m, turned, pair, sems = refs[-7:]
    core, x = lax.axis_index("c"), lax.axis_index("x")
    pairs = ((q, k), (v, m))

    def copies(i, pair_out):
        lanes = HALVES[i]
        return [
            pltpu.make_async_copy(pair.at[pl.ds(320 * j, 320), lanes], out.at[:, lanes], sems.at[i, j])
            for j, out in enumerate(pair_out)
        ]

    z0 = lax.axis_index("z")
    for j, a in enumerate((a0, a1, a2, a3)):
        for r in range(NZ):
            chip = lax.rem(z0 + NZ - r, NZ) * NX + lax.rem(x + NX - j, NX)
            rows = pl.ds(pl.multiple_of(chip * ROWS, 8), ROWS)
            for t in range(COLS):
                tile = a[r, ROWS * t : ROWS * t + ROWS, :]
                turned[rows, LANES * t : LANES * t + LANES] = tile.astype(f32)
    for i in range(2):
        half = slice(640 * i, 640 * i + 640)
        for t in range(COLS):
            lanes = slice(LANES * t, LANES * t + LANES)
            pair[lanes, half] = turned[half, lanes].T.astype(bf16)
        for flip in range(2):

            @pl.when(core == (flip if own else 1 - flip))
            def _(flip=flip):
                for c in copies(i, pairs[flip]):
                    c.start()

    for i in range(2):
        for c in copies(i, pairs[0]):
            c.wait()


def call(kernel, out_shape, in_specs, scratch=(), out_specs=None, aliases={}):
    return pl.pallas_call(
        kernel,
        compiler_params=pltpu.CompilerParams(vmem_limit_bytes=24 << 20),
        out_shape=out_shape,
        in_specs=in_specs,
        out_specs=out_specs or jax.tree.map(lambda _: vmem(1)[0], out_shape),
        input_output_aliases=aliases,
        scratch_shapes=scratch,
    )


def on_device(pq, pk, pv, pm, pn, mq, mk, mv, mm, mn):
    core, x = lax.axis_index("c"), lax.axis_index("x")
    even = core == 0
    pq, pk, pv, pm = pq[0].T, pk[0].T, pv[0].T, pm[0]
    dma = pltpu.SemaphoreType.DMA

    norm = shift(pn, 0, 0, 1)
    norm = pn + norm
    norm = jnp.pad(norm.reshape(NZ, NX, 1, ROWS), ((0, 0), (0, 0), (0, 7), (0, LANES - ROWS)))
    chunks_b, chunks_a = SPLIT // CHUNK, (640 - SPLIT) // CHUNK
    send_b = call(
        pick_kernel, pltpu.VMEM((SPLIT, 1280), f32), hbm(2), [dma((chunks_b,))]
    )(*far(pq, pv))
    got_b = shift(send_b, 0, 0, 1)
    send_a = call(
        pick_kernel, pltpu.VMEM((640 - SPLIT, 1280), f32), hbm(4), [dma((chunks_a,))]
    )(*far(pq, pk, pv, pm))
    got_a = shift(send_a, 0, 0, 1)
    heads, tails = jnp.concatenate([mq, mk], 1), jnp.concatenate([mv, mm.T], 1)
    mine, theirs = jnp.where(even, heads, tails), jnp.where(even, tails, heads)
    theirs, other = shift(theirs, 0, 0, 1), shift(mn, 0, 0, 1)
    weight = jnp.where(even, jnp.concatenate([mine, theirs]), jnp.concatenate([theirs, mine]))
    norm_weight = jnp.where(even, jnp.concatenate([mn, other]), jnp.concatenate([other, mn]))
    norm_weight = jnp.pad(norm_weight[None], ((0, 7), (0, LANES - ROWS)))

    a_shape, b_shape = (NZ, A_ROWS, LANES), (NX, B_ROWS, LANES)
    b = call(
        split_b_kernel,
        [FAR(b_shape, f32)] * NZ,
        hbm(2) + vmem(2),
        [pltpu.VMEM((SPLIT, 1280), f32), pltpu.VMEM((NZ, *b_shape), f32), dma((2, chunks_b)), dma((NZ,))],
        hbm(NZ),
    )(*far(pq, pv), *near(got_b, norm))
    got = [b[0]]
    for steps in ((1, 7), (2, 6, 3, 5, 4)):
        got += [shift(b[r], r, 0) for r in steps]
    b = got
    a = call(
        split_a_kernel,
        [FAR(a_shape, f32)] + [pltpu.VMEM(a_shape, f32)] * 3,
        hbm(4) + vmem(1),
        [
            pltpu.VMEM((640 - SPLIT, 1280), f32),
            pltpu.VMEM((4, NX, ROWS, LANES), f32),
            dma((2, chunks_a)),
        ],
    )(*far(pq, pk, pv, pm), *near(got_a))
    a = shift_x(a)
    a, b, weight, norm_weight = lax.optimization_barrier((a, b, weight, norm_weight))
    a = call(
        sum_a_kernel,
        pltpu.VMEM(a_shape, f32),
        hbm(1) + vmem(3),
        [pltpu.VMEM(a_shape, f32), dma((NZ,))],
    )(*far(a[0]), *near(*a[1:]))
    a = spread(a)
    b = call(
        sum_b_kernel,
        [pltpu.VMEM((B_ROWS, LANES), f32)] * NX,
        hbm(1) + vmem(NZ - 1),
        [pltpu.VMEM(b_shape, f32), dma],
    )(*far(b[0]), *near(*b[1:]))
    b = [b[0]] + [shift(b[j], 0, j) for j in (1, 2, 3)]
    a, stepped, stepped_norm = call(
        step_kernel,
        [
            pltpu.VMEM((G_ROWS, LANES), bf16),
            pltpu.VMEM((ROWS, 640), f32),
            pltpu.VMEM((8, LANES), f32),
        ],
        vmem(7),
    )(*near(a, *b, weight, norm_weight))

    by_step = {0: a}
    for steps in ((1, 7), (2, 6, 3, 5, 4)):
        by_step |= {r: shift(a, r, 0) for r in steps}
    a = jnp.stack([by_step[r] for r in range(NZ)])
    a = shift_x([a] * NX)
    stepped_norm = lax.dynamic_slice_in_dim(stepped_norm[0], 20 * core, 20)
    kept = lax.dynamic_slice_in_dim(stepped, 20 * core, 20)
    swapped = shift(lax.dynamic_slice_in_dim(stepped, 20 * (1 - core), 20), 0, 0, 1)
    heads, tails = jnp.where(even, kept, swapped), jnp.where(even, swapped, kept)
    outs = (heads[:, :320], heads[:, 320:], tails[:, :320], tails[:, 320:].T, stepped_norm)
    a[3], outs = lax.optimization_barrier((a[3], outs))
    other_a = [shift(v, 0, 0, 1) for v in a]
    own_x = jnp.arange(NX)[:, None]
    norm = sum(
        jnp.where(own_x == lax.rem(x + NX - j, NX), v[:, None, G_ROWS - 8, :ROWS], 0) for j, v in enumerate(a)
    )
    norm = jnp.concatenate([norm[:1], norm[:0:-1]])
    place = lax.rem(NZ - lax.axis_index("z"), NZ)
    norm = lax.dynamic_slice_in_dim(jnp.concatenate([norm, norm]), place, NZ)
    scratch = [pltpu.VMEM((1280, 640), f32), pltpu.VMEM((640, 1280), bf16), dma((2, 2))]
    outs_shape = [FAR((320, 1280), bf16)] * 4
    half = call(partial(turn_kernel, True), outs_shape, vmem(4), scratch, hbm(4))(*near(*a))
    aliases = {4 + i: i for i in range(4)}
    q, k, v, m = call(
        partial(turn_kernel, False), outs_shape, vmem(4) + hbm(4), scratch, hbm(4), aliases
    )(*near(*other_a), *half)
    return (q.T, k.T, v.T, m, norm.reshape(-1).astype(bf16), *outs)


def solution(mesh):
    split = Mesh(mesh.devices.reshape(NZ, NX, NC, -1), ("z", "x", "c", "model"))
    r = CHIPS
    in_specs = (
        (P(r, None, "model"),) * 3
        + (P(r, "model", None), P(r, None))
        + (P(r, "model"),) * 3
        + (P("model", r), P(r))
    )
    out_specs = (
        (P(None, "model"),) * 3
        + (P("model", None), P())
        + (P(r, "model"),) * 3
        + (P("model", r), P(r))
    )
    return jax.shard_map(
        on_device, mesh=split, in_specs=in_specs, out_specs=out_specs, check_vma=False
    )
```

```python
from functools import partial

import jax
import jax.numpy as jnp
from jax import lax
from jax.experimental import pallas as pl
from jax.experimental.pallas import tpu as pltpu
from jax.sharding import Mesh
from jax.sharding import PartitionSpec as P


learn_rate = 0.3
NZ, NX, NC = 8, 4, 2
CHIPS = ("z", "x", "c")
f32, bf16 = jnp.float32, jnp.bfloat16
ROWS, LANES, COLS = 40, 128, 5
A_ROWS, B_ROWS, SPLIT = 4 * ROWS, ROWS + 8, LANES
G_ROWS = COLS * ROWS + 8
CHUNK = 32


def shift(v, dz, dx, dc=0):
    pairs = []
    for z in range(NZ):
        for x in range(NX):
            for c in range(NC):
                there = ((z + dz) % NZ * NX + (x + dx) % NX) * NC + (c ^ dc)
                pairs.append(((z * NX + x) * NC + c, there))
    return lax.ppermute(v, CHIPS, pairs)


def shift_x(v):
    near_ones = shift(v[1], 0, 1), shift(v[3], 0, 3)
    return [v[0], near_ones[0], shift(v[2], 0, 2), near_ones[1]]


def shift_z(v):
    out = []
    for steps in ((1, 7), (2, 6, 3, 5, 4)):
        out += [shift(v[r], r, 0) for r in steps]
    return out


def block_copies(blocks, out, sems, lanes=pl.ds(0, 1280)):
    copies, at = [], 0
    for source, low, count in blocks:
        for r in range(0, count, CHUNK):
            rows, place = pl.ds(low + r, CHUNK), pl.ds(at, CHUNK)
            copies.append(pltpu.make_async_copy(source.at[rows, lanes], out.at[place, lanes], sems.at[at // CHUNK]))
            at += CHUNK
    return copies


def start_for(wanted, pairs, copies_of):
    for core in range(NC):

        @pl.when(lax.axis_index("c") == core)
        def _(core=core):
            for c in copies_of(pairs[wanted(core)]):
                c.start()


def blocks_b(q, v):
    return [[(q, 0, SPLIT)], [(v, 0, SPLIT)]]


def blocks_a(q, k, v, m):
    rest = 320 - SPLIT
    return [[(q, SPLIT, rest), (k, 0, 320)], [(v, SPLIT, rest), (m, 0, 320)]]


def pick_kernel(*refs):
    *sources, send, sems = refs
    pairs = (blocks_b if len(sources) == 2 else blocks_a)(*sources)
    copies_of = lambda blocks: block_copies(blocks, send, sems)
    start_for(lambda core: 1 - core, pairs, copies_of)
    for c in copies_of(pairs[0]):
        c.wait()


HALVES = (pl.ds(0, 640), pl.ds(640, 640))


def split_b_kernel(q, v, got, norm, *refs):
    *outs, own, b, sems, out_sems = refs
    z0 = lax.axis_index("z")
    pairs = blocks_b(q, v)
    halves = lambda blocks: [block_copies(blocks, own, sems.at[i], HALVES[i]) for i in range(2)]
    start_for(lambda core: core, pairs, lambda blocks: sum(halves(blocks), []))
    steps = [lax.rem(z + NZ - z0, NZ) for z in range(NZ)]
    for z, step in enumerate(steps):
        b[step, :, B_ROWS - 8 :, :] = norm[z]
    for i, copies in enumerate(halves(pairs[0])):
        for c in copies:
            c.wait()
        lanes = slice(640 * i, 640 * i + 640)
        tile = (own[:, lanes] + got[:, lanes]).T.reshape(4, NX, ROWS, LANES)
        for z in range(4):
            b[steps[4 * i + z], :, :ROWS, :] = tile[z]
    out_copies = [pltpu.make_async_copy(b.at[r], outs[r], out_sems.at[r]) for r in range(NZ)]
    for c in out_copies:
        c.start()
    for c in out_copies:
        c.wait()


def split_a_kernel(q, k, v, m, got, a0, a1, a2, a3, own, turned, sems):
    x = lax.axis_index("x")
    pairs = blocks_a(q, k, v, m)
    halves = lambda blocks: [block_copies(blocks, own, sems.at[i], HALVES[i]) for i in range(2)]
    start_for(lambda core: core, pairs, lambda blocks: sum(halves(blocks), []))
    for i, copies in enumerate(halves(pairs[0])):
        lanes = slice(640 * i, 640 * i + 640)
        for t in range(COLS - 1):
            rows = slice(LANES * t, LANES * t + LANES)
            for c in copies[LANES // CHUNK * t : LANES // CHUNK * (t + 1)]:
                c.wait()
            turned[...] = (own[rows, lanes] + got[rows, lanes]).T.reshape(4, NX, ROWS, LANES)
            for j, a in enumerate((a0, a1, a2, a3)):
                a[4 * i : 4 * i + 4, ROWS * t : ROWS * t + ROWS, :] = turned[:, lax.rem(x + j, NX)]


def vmem(n):
    return [pl.BlockSpec(memory_space=pltpu.VMEM)] * n


def hbm(n):
    return [pl.BlockSpec(memory_space=pltpu.HBM)] * n


FAR = pltpu.HBM


def near(*arrays):
    return [pltpu.with_memory_space_constraint(v, pltpu.VMEM) for v in arrays]


def far(*arrays):
    return [pltpu.with_memory_space_constraint(v, pltpu.HBM) for v in arrays]


def sum_a_kernel(a0, a1, a2, a3, *refs):
    *outs, own, sems = refs
    places = [lax.rem(lax.axis_index("z") + r, NZ) for r in range(NZ)]
    copies = [pltpu.make_async_copy(a0.at[z], own.at[r], sems.at[r]) for r, z in enumerate(places)]
    for c in copies:
        c.start()
    for r, z in enumerate(places):
        copies[r].wait()
        outs[r][...] = own[r] + a1[z] + a2[z] + a3[z]


def sum_b_kernel(*refs):
    first, rest, outs, own, sem = refs[0], refs[1:NZ], refs[NZ:-2], refs[-2], refs[-1]
    x = lax.axis_index("x")
    copy = pltpu.make_async_copy(first, own, sem)
    copy.start()
    copy.wait()
    for j, out in enumerate(outs):
        at = lax.rem(x + j, NX)
        total = own[at]
        for b in rest:
            total = total + b[at]
        out[...] = total


def step_kernel(*refs):
    a, (b0, b1, b2, b3, weight, norm_weight, out, stepped, stepped_norm) = refs[:NZ], refs[NZ:]
    rate = (NZ * NX * NC) ** (-0.5)
    total_a = a[0][...]
    for r in range(1, NZ):
        total_a = total_a + a[r][...]
    total_b = b0[...] + b1[...] + b2[...] + b3[...]
    for t in range(COLS):
        lanes = slice(LANES * t, LANES * t + LANES)
        total = total_b[:ROWS] if t == 0 else total_a[ROWS * (t - 1) : ROWS * t]
        stepped[:, lanes] = weight[:, lanes] - learn_rate * (total * rate)
    stepped_norm[...] = norm_weight[...] - learn_rate * (total_b[B_ROWS - 8 :] * rate)
    for t in range(COLS):
        out[ROWS * t : ROWS * t + ROWS] = stepped[:, LANES * t : LANES * t + LANES].astype(bf16)
    out[G_ROWS - 8 :] = stepped_norm[...].astype(bf16)


def turn_kernel(own, a0, a1, a2, a3, *refs):
    q, k, v, m, turned, pair, sems = refs[-7:]
    core, x = lax.axis_index("c"), lax.axis_index("x")
    pairs = ((q, k), (v, m))

    def copies(i, pair_out):
        lanes = HALVES[i]
        return [
            pltpu.make_async_copy(pair.at[pl.ds(320 * j, 320), lanes], out.at[:, lanes], sems.at[i, j])
            for j, out in enumerate(pair_out)
        ]

    z0 = lax.axis_index("z")
    for j, a in enumerate((a0, a1, a2, a3)):
        for r in range(NZ):
            chip = lax.rem(z0 + NZ - r, NZ) * NX + lax.rem(x + NX - j, NX)
            rows = pl.ds(pl.multiple_of(chip * ROWS, 8), ROWS)
            for t in range(COLS):
                tile = a[r, ROWS * t : ROWS * t + ROWS, :]
                turned[rows, LANES * t : LANES * t + LANES] = tile.astype(f32)
    for i in range(2):
        half = slice(640 * i, 640 * i + 640)
        for t in range(COLS):
            lanes = slice(LANES * t, LANES * t + LANES)
            pair[lanes, half] = turned[half, lanes].T.astype(bf16)
        for flip in range(2):

            @pl.when(core == (flip if own else 1 - flip))
            def _(flip=flip):
                for c in copies(i, pairs[flip]):
                    c.start()

    for i in range(2):
        for c in copies(i, pairs[0]):
            c.wait()


def call(kernel, out_shape, in_specs, scratch=(), out_specs=None, aliases={}):
    return pl.pallas_call(
        kernel,
        compiler_params=pltpu.CompilerParams(vmem_limit_bytes=24 << 20),
        out_shape=out_shape,
        in_specs=in_specs,
        out_specs=out_specs or jax.tree.map(lambda _: vmem(1)[0], out_shape),
        input_output_aliases=aliases,
        scratch_shapes=scratch,
    )


def on_device(pq, pk, pv, pm, pn, mq, mk, mv, mm, mn):
    core, x = lax.axis_index("c"), lax.axis_index("x")
    even = core == 0
    pq, pk, pv, pm = pq[0].T, pk[0].T, pv[0].T, pm[0]
    dma = pltpu.SemaphoreType.DMA

    norm = shift(pn, 0, 0, 1)
    norm = pn + norm
    norm = jnp.pad(norm.reshape(NZ, NX, 1, ROWS), ((0, 0), (0, 0), (0, 7), (0, LANES - ROWS)))
    chunks_b, chunks_a = SPLIT // CHUNK, (640 - SPLIT) // CHUNK
    send_b = call(
        pick_kernel, pltpu.VMEM((SPLIT, 1280), f32), hbm(2), [dma((chunks_b,))]
    )(*far(pq, pv))
    got_b = shift(send_b, 0, 0, 1)
    send_a = call(
        pick_kernel, pltpu.VMEM((640 - SPLIT, 1280), f32), hbm(4), [dma((chunks_a,))]
    )(*far(pq, pk, pv, pm))
    got_a = shift(send_a, 0, 0, 1)
    heads, tails = jnp.concatenate([mq, mk], 1), jnp.concatenate([mv, mm.T], 1)
    mine, theirs = jnp.where(even, heads, tails), jnp.where(even, tails, heads)
    theirs, other = shift(theirs, 0, 0, 1), shift(mn, 0, 0, 1)
    weight = jnp.where(even, jnp.concatenate([mine, theirs]), jnp.concatenate([theirs, mine]))
    norm_weight = jnp.where(even, jnp.concatenate([mn, other]), jnp.concatenate([other, mn]))
    norm_weight = jnp.pad(norm_weight[None], ((0, 7), (0, LANES - ROWS)))

    a_shape, b_shape = (NZ, A_ROWS, LANES), (NX, B_ROWS, LANES)
    b = call(
        split_b_kernel,
        [FAR(b_shape, f32)] * NZ,
        hbm(2) + vmem(2),
        [pltpu.VMEM((SPLIT, 1280), f32), pltpu.VMEM((NZ, *b_shape), f32), dma((2, chunks_b)), dma((NZ,))],
        hbm(NZ),
    )(*far(pq, pv), *near(got_b, norm))
    got = [b[0]]
    for steps in ((1, 7), (2, 6, 3, 5, 4)):
        got += [shift(b[r], r, 0) for r in steps]
    b = got
    a = call(
        split_a_kernel,
        [FAR(a_shape, f32)] + [pltpu.VMEM(a_shape, f32)] * 3,
        hbm(4) + vmem(1),
        [
            pltpu.VMEM((640 - SPLIT, 1280), f32),
            pltpu.VMEM((4, NX, ROWS, LANES), f32),
            dma((2, chunks_a)),
        ],
    )(*far(pq, pk, pv, pm), *near(got_a))
    a = shift_x(a)
    a, b, weight, norm_weight = lax.optimization_barrier((a, b, weight, norm_weight))
    a = call(
        sum_a_kernel,
        [pltpu.VMEM((A_ROWS, LANES), f32)] * NZ,
        hbm(1) + vmem(3),
        [pltpu.VMEM(a_shape, f32), dma((NZ,))],
    )(*far(a[0]), *near(*a[1:]))
    a = [a[0]] + shift_z(a)
    b = call(
        sum_b_kernel,
        [pltpu.VMEM((B_ROWS, LANES), f32)] * NX,
        hbm(1) + vmem(NZ - 1),
        [pltpu.VMEM(b_shape, f32), dma],
    )(*far(b[0]), *near(*b[1:]))
    b = shift_x(b)
    a, stepped, stepped_norm = call(
        step_kernel,
        [
            pltpu.VMEM((G_ROWS, LANES), bf16),
            pltpu.VMEM((ROWS, 640), f32),
            pltpu.VMEM((8, LANES), f32),
        ],
        vmem(NZ + 6),
    )(*near(*a, *b, weight, norm_weight))

    by_step = {0: a}
    for steps in ((1, 7), (2, 6, 3, 5, 4)):
        by_step |= {r: shift(a, r, 0) for r in steps}
    a = jnp.stack([by_step[r] for r in range(NZ)])
    a = shift_x([a] * NX)
    stepped_norm = lax.dynamic_slice_in_dim(stepped_norm[0], 20 * core, 20)
    kept = lax.dynamic_slice_in_dim(stepped, 20 * core, 20)
    swapped = shift(lax.dynamic_slice_in_dim(stepped, 20 * (1 - core), 20), 0, 0, 1)
    heads, tails = jnp.where(even, kept, swapped), jnp.where(even, swapped, kept)
    outs = (heads[:, :320], heads[:, 320:], tails[:, :320], tails[:, 320:].T, stepped_norm)
    a[3], outs = lax.optimization_barrier((a[3], outs))
    other_a = [shift(v, 0, 0, 1) for v in a]
    own_x = jnp.arange(NX)[:, None]
    norm = sum(
        jnp.where(own_x == lax.rem(x + NX - j, NX), v[:, None, G_ROWS - 8, :ROWS], 0) for j, v in enumerate(a)
    )
    norm = jnp.concatenate([norm[:1], norm[:0:-1]])
    place = lax.rem(NZ - lax.axis_index("z"), NZ)
    norm = lax.dynamic_slice_in_dim(jnp.concatenate([norm, norm]), place, NZ)
    scratch = [pltpu.VMEM((1280, 640), f32), pltpu.VMEM((640, 1280), bf16), dma((2, 2))]
    outs_shape = [FAR((320, 1280), bf16)] * 4
    half = call(partial(turn_kernel, True), outs_shape, vmem(4), scratch, hbm(4))(*near(*a))
    aliases = {4 + i: i for i in range(4)}
    q, k, v, m = call(
        partial(turn_kernel, False), outs_shape, vmem(4) + hbm(4), scratch, hbm(4), aliases
    )(*near(*other_a), *half)
    return (q.T, k.T, v.T, m, norm.reshape(-1).astype(bf16), *outs)


def solution(mesh):
    split = Mesh(mesh.devices.reshape(NZ, NX, NC, -1), ("z", "x", "c", "model"))
    r = CHIPS
    in_specs = (
        (P(r, None, "model"),) * 3
        + (P(r, "model", None), P(r, None))
        + (P(r, "model"),) * 3
        + (P("model", r), P(r))
    )
    out_specs = (
        (P(None, "model"),) * 3
        + (P("model", None), P())
        + (P(r, "model"),) * 3
        + (P("model", r), P(r))
    )
    return jax.shard_map(
        on_device, mesh=split, in_specs=in_specs, out_specs=out_specs, check_vma=False
    )
```
